32 devices in a mesh: row: 4 (over z), col: 8 (over y, x, core).
Axes of the slice: x: 2, y: 2, z: 4, core: 2. Of those that a mesh axis runs over, the one named last changes fastest.
Arguments:
- front_matrix: bfloat16 [32768, 32768], P('row', 'col'), may hold values from -0.03125 to 0.03125
- right_random: bfloat16 [32768, 128], P(('col', 'row')), may hold values from -32 to 32
- left_random: bfloat16 [32768, 128], P(('row', 'col')), may hold values from -32 to 32
- row_basis: bfloat16 [32768, 384], P('row'), may hold values from -1 to 1, as said below
- column_basis: bfloat16 [32768, 384], P('col'), may hold values from -1 to 1, as said below
Outputs:
- row_samples: float32 [128, 32768], P('col', 'row')
- column_samples: float32 [128, 32768], P('row', 'col')
- row_spread: float32 [64], P('row')
- column_spread: float32 [64], P('col')
The draws below stay inside these ranges and needn't reach their ends.
Inputs may be any that keep to these rules, and one draw needn't show every extreme that they name: Within each leaf node's 512 rows, the columns of row_basis are orthonormal up to their rounding to bfloat16. Within each leaf node's 512 rows, the columns of column_basis are orthonormal up to their rounding to bfloat16.
All inputs are finite; a program needn't handle non-finite values.
Results may differ from the reference program's by a relative error of at most 0.0003.
Values may be sent and summed in bfloat16 or wider, within the bound.
No kernel may reach another device: no remote copies, remote signals or barrier semaphores. Data moves between devices by JAX's collectives and lax.ppermute only.
A program may use at most 128 MiB of HBM per device.

```python
import jax
import jax.numpy as jnp
from jax import lax

N = 32768
SAMPLES = 128
EARLIER = 384
NODE = 512


def node_orthonormal(key):
    normals = jax.random.normal(key, (N // NODE, NODE, EARLIER), jnp.float32)
    factors, _ = jnp.linalg.qr(normals)
    return factors.reshape(N, EARLIER).astype(jnp.bfloat16)


def rising_block(key):
    position = jnp.arange(SAMPLES, dtype=jnp.float32) / (SAMPLES - 1)
    entries = jnp.clip(jax.random.normal(key, (N, SAMPLES), jnp.float32), -4.0, 4.0)
    scales = jnp.exp(position * jnp.log(4.0))
    return (entries * scales[None, :]).astype(jnp.bfloat16)


def draw_right_random(key, part):
    return rising_block(jax.random.fold_in(key, 41))


def draw_left_random(key, part):
    return rising_block(jax.random.fold_in(key, 53))


def draw_row_basis(key, part):
    return node_orthonormal(jax.random.fold_in(key, 11))


def draw_column_basis(key, part):
    return node_orthonormal(jax.random.fold_in(key, 29))


def block_scale(own_key, dims, cuts, smallest, high):
    def one(dim, blocks):
        draws = jax.random.uniform(jax.random.fold_in(jax.random.fold_in(own_key, 6), dim), (blocks,), jnp.float32, smallest / len(cuts), high / len(cuts))
        return jnp.repeat(jnp.exp(draws), dims[dim] // blocks).reshape((-1,) + (1,) * (len(dims) - dim - 1))

    loudness = one(*cuts[0])
    for cut in cuts[1:]:
        loudness = loudness * one(*cut)
    return loudness


def normal_values(key, dims, spread, reach, pieces=(), held_as=jnp.bfloat16):
    drawn = spread * jax.random.normal(key, dims, jnp.float32)
    if pieces:
        drawn = drawn * block_scale(key, dims, pieces, -0.22, 0.18)
    return jnp.clip(drawn, -reach, reach).astype(held_as)


def setup_inputs(seed: int = 0) -> dict:
    splits = jax.random.split(jax.random.key(seed), 6)
    front_matrix = normal_values(splits[0], (N, N), N ** -0.5, 0.03125, ((0, 4), (1, 8)))
    right_random = draw_right_random(jax.random.fold_in(splits[5], 71), 0)
    left_random = draw_left_random(jax.random.fold_in(splits[5], 71), 0)
    row_basis = draw_row_basis(jax.random.fold_in(splits[5], 71), 0)
    column_basis = draw_column_basis(jax.random.fold_in(splits[5], 71), 0)
    return {"front_matrix": front_matrix, "right_random": right_random, "left_random": left_random, "row_basis": row_basis, "column_basis": column_basis}


def project_out(full_samples, basis):
    count = full_samples.shape[0]
    nodes = basis.shape[0] // NODE
    shaped = full_samples.astype(jnp.float32).reshape(count, nodes, NODE)
    stacked = basis.astype(jnp.float32).reshape(nodes, NODE, EARLIER)
    coeffs = jnp.einsum('knr,nre->kne', shaped, stacked, precision=lax.Precision.HIGHEST)
    correction = jnp.einsum('kne,nre->knr', coeffs, stacked, precision=lax.Precision.HIGHEST)
    cleaned = shaped - correction
    squares = lax.optimization_barrier(jnp.sum(cleaned * cleaned, axis=(0, 2)))
    return (cleaned.reshape(count, nodes * NODE), jnp.sqrt(squares / (SAMPLES * NODE)))

def reference(front_matrix, right_random, left_random, row_basis, column_basis):
    row_full = jnp.dot(front_matrix.astype(jnp.float32), right_random.astype(jnp.float32), preferred_element_type=jnp.float32).T
    column_full = jnp.dot(left_random.T.astype(jnp.float32), front_matrix.astype(jnp.float32), preferred_element_type=jnp.float32)
    row_samples, row_spread = project_out(row_full, row_basis)
    column_samples, column_spread = project_out(column_full, column_basis)
    return (row_samples, column_samples, row_spread, column_spread)
```

```python
import functools

import jax
import jax.numpy as jnp
from jax import lax
from jax.experimental import pallas as pl
from jax.experimental.pallas import tpu as pltpu
from jax.sharding import PartitionSpec as P

NODE = 512
CHUNKS = 1


def xor_send(x, n, bits):
    return lax.ppermute(x, "col", [(i, i ^ bits) for i in range(n)])


def shift_send(x, n, step):
    return lax.ppermute(x, "row", [(i, (i + step) % n) for i in range(n)])


def ring_gather(x, n):
    if n != 4:
        return [x] + [shift_send(x, n, d) for d in range(1, n)]
    half = x.shape[0] // 2
    before, after = shift_send(x, n, 1), shift_send(x, n, 3)
    far = jnp.concatenate([shift_send(before[:half], n, 1), shift_send(after[half:], n, 3)], 0)
    return [x, before, far, after]


def nt(a, b):
    return lax.dot_general(a, b, (((1,), (1,)), ((), ())), preferred_element_type=jnp.float32)


def nn(a, b):
    return lax.dot_general(a, b, (((1,), (0,)), ((), ())), preferred_element_type=jnp.float32)


def products_kernel(where, front, *refs, n_row, n_col, first_block, has_acc):
    rights, refs = refs[:n_row], refs[n_row:]
    lefts, refs = refs[:n_col], refs[n_col:]
    if has_acc:
        accs, refs = refs[:n_row], refs[n_row:]
    keep, send = refs[:2]
    columns = refs[2 : 2 + n_row]
    right_all, left_all = refs[2 + n_row :]
    step = pl.program_id(0)
    block = front.shape[0]
    wide = right_all.shape[2]
    tall = left_all.shape[2]
    my_row, my_col = where[0], where[1]

    @pl.when(step == 0)
    def _():
        for d in range(n_row):
            right_all[lax.rem(my_row - d + n_row, n_row)] = rights[d][...]
        for p in range(n_col):
            left_all[my_col ^ p] = lefts[p][...]
        for d in range(n_row):
            columns[d][...] = accs[d][...] if has_acc else jnp.zeros(columns[d].shape, jnp.float32)

    at = (step + first_block) * block
    shard = lax.div(at, tall)
    if tall == block:
        left = left_all[shard]
    else:
        left = left_all[shard, :, pl.ds(pl.multiple_of(lax.rem(at, tall), block), block)]
    each = left.shape[0] // n_row
    row = tall_row = None
    for s in range(n_row):
        tile = front[:, s * wide : (s + 1) * wide]
        if s % 2:
            part = nt(right_all[s], tile)
            row = part if row is None else row + part
        else:
            part = nt(tile, right_all[s])
            tall_row = part if tall_row is None else tall_row + part
        col = nn(left, tile)
        for d in range(n_row):
            columns[d][:, s * wide : (s + 1) * wide] += col[d * each : (d + 1) * each]
    row = row + tall_row.T
    half = row.shape[0] // 2
    keep[...] = row[:half]
    send[...] = row[half:]


def products(where, front, rights, lefts, accs, chunk, n_row, n_col):
    rows, cols = front.shape
    count, wide = rights[0].shape
    tall = lefts[0].shape[1]
    block = min(512, tall)
    steps = rows // CHUNKS // block
    first = chunk * steps
    whole = lambda shape: pl.BlockSpec(shape, lambda i, w: (0,) * len(shape))
    each = count // n_row
    col_spec = whole((each, cols))
    row_spec = pl.BlockSpec((count // 2, block), lambda i, w: (0, i))
    outs = pl.pallas_call(
        functools.partial(products_kernel, n_row=n_row, n_col=n_col, first_block=first, has_acc=accs is not None),
        grid_spec=pltpu.PrefetchScalarGridSpec(
            num_scalar_prefetch=1,
            grid=(steps,),
            in_specs=[pl.BlockSpec((block, cols), lambda i, w: (i + first, 0))]
            + [whole((count, wide))] * n_row
            + [whole((count, tall))] * n_col
            + ([col_spec] * n_row if accs is not None else []),
            out_specs=[row_spec] * 2 + [col_spec] * n_row,
            scratch_shapes=[pltpu.VMEM((n_row, count, wide), jnp.bfloat16), pltpu.VMEM((n_col, count, tall), jnp.bfloat16)],
        ),
        out_shape=[jax.ShapeDtypeStruct((count // 2, steps * block), jnp.float32)] * 2
        + [jax.ShapeDtypeStruct((each, cols), jnp.float32)] * n_row,
        cost_estimate=pl.CostEstimate(flops=4 * count * rows * cols // CHUNKS, bytes_accessed=2 * rows * cols // CHUNKS, transcendentals=0),
        compiler_params=pltpu.CompilerParams(dimension_semantics=("arbitrary",), vmem_limit_bytes=48 * 2**20),
        name="products",
    )(where, front, *rights, *lefts, *(accs or ()))
    return outs[0], outs[1], list(outs[2:])


def three_way(x):
    high = x.astype(jnp.bfloat16)
    rest = x - high.astype(jnp.float32)
    mid = rest.astype(jnp.bfloat16)
    low = (rest - mid.astype(jnp.float32)).astype(jnp.bfloat16)
    return high, mid, low


def exact_dot(dot, x, basis):
    rows = x.shape[0]
    pad = (-rows) % 16
    if pad:
        x = jnp.concatenate([x, jnp.zeros((pad, x.shape[1]), x.dtype)], 0)
    full = rows + pad
    out = dot(jnp.concatenate(three_way(x), 0), basis)
    return (out[:full] + out[full : 2 * full] + out[2 * full :])[:rows]


def project_kernel(basis, *refs):
    pieces, (out, squares) = refs[:-2], refs[-2:]
    spans = [slice(n * NODE, (n + 1) * NODE) for n in range(basis.shape[0] // NODE)]
    fulls = [sum(piece[:, span] for piece in pieces) for span in spans]
    coeffs = [exact_dot(nn, full, basis[span, :]) for full, span in zip(fulls, spans)]
    fixes = [exact_dot(nt, coeff, basis[span, :]) for coeff, span in zip(coeffs, spans)]
    for n, span in enumerate(spans):
        cleaned = fulls[n] - fixes[n]
        out[:, span] = cleaned
        squares[n : n + 1, 0, :] = jnp.sum(cleaned * cleaned, axis=0, keepdims=True)


def project(basis, pieces, first_node):
    count, length = pieces[0].shape
    per = max(p for p in (1, 2, 4) if (length // NODE) % p == 0)
    steps = length // NODE // per
    skip = first_node // per
    spec = pl.BlockSpec((count, per * NODE), lambda i: (0, i))
    return pl.pallas_call(
        project_kernel,
        grid=(steps,),
        in_specs=[pl.BlockSpec((per * NODE, basis.shape[1]), lambda i: (i + skip, 0))] + [spec] * len(pieces),
        out_specs=[spec, pl.BlockSpec((per, 1, NODE), lambda i: (i, 0, 0))],
        out_shape=[
            jax.ShapeDtypeStruct((count, length), jnp.float32),
            jax.ShapeDtypeStruct((length // NODE, 1, NODE), jnp.float32),
        ],
        cost_estimate=pl.CostEstimate(flops=2**32, bytes_accessed=2**23, transcendentals=0),
        compiler_params=pltpu.CompilerParams(dimension_semantics=("arbitrary",)),
        name="project",
    )(basis, *pieces)


def solution(mesh):
    n_row, n_col = mesh.shape["row"], mesh.shape["col"]
    n_pair = n_col // 2

    def shards(front, right, left, row_basis, column_basis):
        my_row, my_col = lax.axis_index("row"), lax.axis_index("col")
        where = jnp.stack([my_row, my_col]).astype(jnp.int32)
        samples = right.shape[1]
        order = jnp.asarray([2 * q for q in range(n_pair)] + [2 * q + 1 for q in range(n_pair)], jnp.int32)
        right_t = right.T.reshape(n_col, -1)[my_col ^ order].reshape(samples, -1)
        left_t = left.T.reshape(n_row, -1)[(my_row + jnp.arange(n_row)) % n_row].reshape(samples, -1)

        rights = ring_gather(right_t, n_row)
        mine = [left_t] + [xor_send(left_t, n_col, 2 * q) for q in range(1, n_pair)]
        theirs = [xor_send(x, n_col, 1) for x in mine]
        lefts = [x for pair in zip(mine, theirs) for x in pair]

        accs = None
        row_parts = []
        for chunk in range(CHUNKS):
            keep, send, accs = products(where, front, rights, lefts, accs, chunk, n_row, n_col)
            row_parts.append((keep, send))

        each = samples // n_col
        row_outs, row_squares = [], []
        nodes = row_basis.shape[0] // NODE // CHUNKS
        swapped = [xor_send(send, n_col, 1) for _, send in row_parts]
        if n_row == 4:
            half = accs[2].shape[0] // 2
            relays = [shift_send(accs[2][:half], n_row, 1), shift_send(accs[2][half:], n_row, 3)]
            relays, swapped = lax.optimization_barrier((relays, swapped))
            forward = jnp.concatenate([accs[1][:half] + relays[0], accs[1][half:]], 0)
            backward = jnp.concatenate([accs[3][:half], accs[3][half:] + relays[1]], 0)
            col_pieces = [accs[0], shift_send(forward, n_row, 1), shift_send(backward, n_row, 3)]
        else:
            col_pieces = [accs[0]] + [shift_send(accs[d], n_row, d) for d in range(1, n_row)]
        row_pieces = []
        for (keep, _), other in zip(row_parts, swapped):
            groups = [keep[q * each : (q + 1) * each] + other[q * each : (q + 1) * each] for q in range(n_pair)]
            row_pieces.append([groups[0]] + [xor_send(groups[q], n_col, 2 * q) for q in range(1, n_pair)])
        col_pieces, row_pieces = lax.optimization_barrier((col_pieces, row_pieces))
        for chunk, pieces in enumerate(row_pieces):
            out, squares = project(row_basis, pieces, chunk * nodes)
            row_outs.append(out)
            row_squares.append(squares)
        column_samples, column_squares = project(column_basis, col_pieces, 0)
        row_sq = jnp.sum(jnp.concatenate(row_squares, 0), axis=(1, 2))
        col_sq = jnp.sum(column_squares, axis=(1, 2))
        row_sq, col_sq = lax.optimization_barrier((row_sq, col_sq))
        row_total = sum([row_sq] + [xor_send(row_sq, n_col, p) for p in range(1, n_col)])
        col_total = sum([col_sq] + [shift_send(col_sq, n_row, d) for d in range(1, n_row)])
        row_spread = jnp.sqrt(row_total / (samples * NODE))
        column_spread = jnp.sqrt(col_total / (samples * NODE))
        return (row_outs[0] if CHUNKS == 1 else jnp.concatenate(row_outs, 1)), column_samples, row_spread, column_spread

    in_specs = (P("row", "col"), P(("col", "row"), None), P(("row", "col"), None), P("row", None), P("col", None))
    out_specs = (P("col", "row"), P("row", "col"), P("row"), P("col"))
    return jax.shard_map(shards, mesh=mesh, in_specs=in_specs, out_specs=out_specs, check_vma=False)
```
